32 devices in a mesh: wide: 8 (over y, x, core), narrow: 4 (over z).
Axes of the slice: x: 2, y: 2, z: 4, core: 2. Of those that a mesh axis runs over, the one named last changes fastest.
Arguments:
- layer_input: bfloat16 [4, 2048, 2048], P(None, 'wide'), may hold values from -6 to 6
- grad_out: bfloat16 [4, 2048, 2048], P(None, 'wide'), may hold values from -6 to 6
- lengths: int32 [4, 8], replicated, may hold values from 1 to 1024, 2048 in all within a row
- w_query: bfloat16 [2048, 2048], P('wide', 'narrow'), may hold values from -0.125 to 0.125
- w_key: bfloat16 [2048, 1024], P('wide', 'narrow'), may hold values from -0.125 to 0.125
- w_value: bfloat16 [2048, 1024], P('wide', 'narrow'), may hold values from -0.125 to 0.125
- w_out: bfloat16 [2048, 2048], P('narrow', 'wide'), may hold values from -0.75 to 0.75
- w_gate: bfloat16 [2048, 6144], P('wide', 'narrow'), may hold values from -0.125 to 0.125
- w_up: bfloat16 [2048, 6144], P('wide', 'narrow'), may hold values from -0.125 to 0.125
- w_down: bfloat16 [6144, 2048], P('narrow', 'wide'), may hold values from -0.078125 to 0.078125
- gain_attn: float32 [2048], replicated, may hold values from 0.25 to 1.75
- gain_ffn: float32 [2048], replicated, may hold values from 0.25 to 1.75
- gain_query: float32 [128], replicated, may hold values from 0.25 to 1.75
- gain_key: float32 [128], replicated, may hold values from 0.25 to 1.75
Outputs:
- output: bfloat16 [4, 2048, 2048], P(None, 'wide')
- grad_input: float32 [4, 2048, 2048], P(None, 'wide')
- grad_wquery: float32 [2048, 2048], P('wide', 'narrow')
- grad_wkey: float32 [2048, 1024], P('wide', 'narrow')
- grad_wvalue: float32 [2048, 1024], P('wide', 'narrow')
- grad_wout: float32 [2048, 2048], P('narrow', 'wide')
- grad_wgate: float32 [2048, 6144], P('wide', 'narrow')
- grad_wup: float32 [2048, 6144], P('wide', 'narrow')
- grad_wdown: float32 [6144, 2048], P('narrow', 'wide')
- grad_gattn: float32 [2048], replicated
- grad_gffn: float32 [2048], replicated
- grad_gquery: float32 [128], replicated
- grad_gkey: float32 [128], replicated
The draws below stay inside these ranges and needn't reach their ends.
Inputs may be any that keep to these rules, and one draw needn't show every extreme that they name: `lengths`: each row cuts the 2048 tokens of its micro-batch into 8 consecutive pieces in order; pieces 0 to 6 are documents and the last piece is padding. A row's pieces sum to 2048, and its largest piece is exactly 1024.
All inputs are finite; a program needn't handle non-finite values.
Results may differ from the reference program's by a relative error of at most 0.022.
Values may be sent and summed in bfloat16 or wider, within the bound.
A program may use at most 256 MiB of HBM per device.

```python
import math
import jax
import jax.numpy as jnp
import numpy as np
from jax import lax

D = 2048
NH = 16
KV = 8
HD = 128
FF = 6144
MICRO = 4
NDOC = 8
LEN = 2048
MOST = 1024


def block_levels(rng, dims, split, low, largest):
    def one(dim, blocks):
        draws = jax.random.uniform(jax.random.fold_in(jax.random.fold_in(rng, 6), dim), (blocks,), jnp.float32, low / len(split), largest / len(split))
        return jnp.repeat(jnp.exp(draws), dims[dim] // blocks).reshape((-1,) + (1,) * (len(dims) - dim - 1))

    level = one(*split[0])
    for cut in split[1:]:
        level = level * one(*cut)
    return level


def profile(number_of, total, reach, skew):
    portions = [(1 << 20) // math.isqrt(grade ** skew) + 1 for grade in range(2, number_of + 1)]
    spare, counts = total - reach - (number_of - 1), [1] * (number_of - 1)
    while spare > 0:
        free = [i for i in range(number_of - 1) if counts[i] < reach]
        whole, remaining = sum([portions[i] for i in free]), spare
        for i in free:
            extra = min(reach - counts[i], max(1, remaining * portions[i] // whole), spare)
            counts[i] = counts[i] + extra
            spare = spare - extra
    return np.array([reach] + counts)


def uneven_parts(rng, number_of, total, limit, slope):
    if number_of == 2:
        one = jax.random.randint(rng, (), max(1, total - limit), min(limit, total - 1) + 1)
        return jnp.stack([one, total - one])
    tallies = jnp.asarray(profile(number_of, total, limit, slope), jnp.int32)
    couples = (number_of - 1) // 2
    donor, sink = tallies[1:1 + 2 * couples:2], tallies[2:2 + 2 * couples:2]
    room = jnp.minimum(donor - 1, limit - sink)
    moved = jax.random.randint(jax.random.fold_in(rng, 1), (couples,), 0, 1 << 20) % (room + 1)
    tallies = tallies.at[1:1 + 2 * couples:2].set(donor - moved).at[2:2 + 2 * couples:2].set(sink + moved)
    return tallies[jax.random.permutation(jax.random.fold_in(rng, 2), number_of)]


def noise(own_key, extent, spread, bound, cuts=(), held_as=jnp.bfloat16):
    level = block_levels(own_key, extent, cuts, -0.22, 0.18) if cuts else 1.0
    array = jax.random.normal(own_key, extent, jnp.float32) * spread * level
    return jnp.minimum(jnp.maximum(array, -bound), bound).astype(held_as)


def setup_inputs(seed: int = 0) -> dict:
    streams_of = jax.random.split(jax.random.key(seed), 15)
    return {
        "layer_input": noise(streams_of[0], (MICRO, LEN, D), 1.0, 6.0, ((1, 8),)),
        "grad_out": noise(streams_of[1], (MICRO, LEN, D), 1.0, 6.0, ((1, 8),)),
        "lengths": jax.vmap(lambda own: uneven_parts(own, NDOC, LEN, MOST, 2))(jax.random.split(streams_of[2], MICRO)).reshape((MICRO, NDOC)).astype(jnp.int32),
        "w_query": noise(streams_of[3], (D, NH * HD), D ** -0.5, 0.125, ((0, 8), (1, 4))),
        "w_key": noise(streams_of[4], (D, KV * HD), D ** -0.5, 0.125, ((0, 8), (1, 4))),
        "w_value": noise(streams_of[5], (D, KV * HD), D ** -0.5, 0.125, ((0, 8), (1, 4))),
        "w_out": noise(streams_of[6], (NH * HD, D), (NH * HD // 32) ** -0.5, 0.75, ((0, 4), (1, 8))),
        "w_gate": noise(streams_of[7], (D, FF), D ** -0.5, 0.125, ((0, 8), (1, 4))),
        "w_up": noise(streams_of[8], (D, FF), D ** -0.5, 0.125, ((0, 8), (1, 4))),
        "w_down": noise(streams_of[9], (FF, D), FF ** -0.5, 0.078125, ((0, 4), (1, 8))),
        "gain_attn": jnp.clip(1.0 + 0.15 * jax.random.normal(streams_of[10], (D,), jnp.float32), 0.25, 1.75),
        "gain_ffn": jnp.clip(1.0 + 0.15 * jax.random.normal(streams_of[11], (D,), jnp.float32), 0.25, 1.75),
        "gain_query": jnp.clip(1.0 + 0.15 * jax.random.normal(streams_of[12], (HD,), jnp.float32), 0.25, 1.75),
        "gain_key": jnp.clip(1.0 + 0.15 * jax.random.normal(streams_of[13], (HD,), jnp.float32), 0.25, 1.75),
    }


@jax.custom_vjp
def low(v):
    return lax.optimization_barrier(v.astype(jnp.bfloat16)).astype(jnp.float32)

@jax.custom_vjp
def low_back(v):
    return v

def low_keep(v):
    return (low(v), None)

def low_pass(kept, grad):
    return (grad,)

def back_keep(v):
    return (v, None)

def back_low(kept, grad):
    return (low(grad),)
low.defvjp(low_keep, low_pass)
low_back.defvjp(back_keep, back_low)
EPSILON = 1e-06
THETA = 1000000.0
HIGHEST = lax.Precision.HIGHEST

def rms_norm(values, gain):
    return values * lax.rsqrt(lax.optimization_barrier(jnp.mean(values * values, axis=-1, keepdims=True)) + EPSILON) * gain

def rotate(values, cosine, sine):
    midway = values.shape[-1] // 2
    turned = jnp.concatenate([-values[..., midway:], values[..., :midway]], axis=-1)
    return values * cosine + turned * sine

def layout(lengths_row, total):
    finish = jnp.cumsum(lengths_row).astype(jnp.int32)
    starts = (finish - lengths_row).astype(jnp.int32)
    places = jnp.arange(total, dtype=jnp.int32)
    segment = lax.optimization_barrier(jnp.sum((places[:, None] >= finish[None, :]).astype(jnp.int32), axis=1)).astype(jnp.int32)
    member = segment[:, None] == jnp.arange(finish.shape[0], dtype=jnp.int32)[None, :]
    opening = lax.optimization_barrier(jnp.sum(jnp.where(member, starts[None, :], 0), axis=1)).astype(jnp.int32)
    return (segment, (places - opening).astype(jnp.int32))

def angles(place):
    frequency = jnp.exp(-math.log(THETA) * jnp.arange(0, HD, 2).astype(jnp.float32) / HD)
    turning = place.astype(jnp.float32)[:, None] * frequency[None, :]
    turning = jnp.concatenate([turning, turning], axis=-1)
    return (jnp.cos(turning), jnp.sin(turning))

def allowed(query_seg, query_idx, key_seg, key_idx):
    same_doc = query_seg[:, None] == key_seg[None, :]
    causal = key_idx[None, :] <= query_idx[:, None]
    usable = (key_seg[None, :] != NDOC - 1) | (key_idx[None, :] == query_idx[:, None])
    return same_doc & causal & usable

def forward_one(row_input, params, segment, place):
    w_query, w_key, w_value, w_out, w_gate, w_up, w_down, gain_attn, gain_ffn, gain_query, gain_key = params
    total = row_input.shape[0]
    factor = 1.0 / math.sqrt(HD)
    cosine, sine = angles(place)
    hidden_one = low(rms_norm(row_input, gain_attn))
    queries = low_back(jnp.dot(hidden_one, w_query, precision=HIGHEST)).reshape(total, NH, HD)
    keys = low_back(jnp.dot(hidden_one, w_key, precision=HIGHEST)).reshape(total, KV, HD)
    values = low(low_back(jnp.dot(hidden_one, w_value, precision=HIGHEST))).reshape(total, KV, HD)
    query_rot = low(rotate(rms_norm(queries, gain_query), cosine[:, None, :], sine[:, None, :]))
    key_rot = low(rotate(rms_norm(keys, gain_key), cosine[:, None, :], sine[:, None, :]))
    key_rep = jnp.repeat(key_rot, NH // KV, axis=1)
    value_rep = jnp.repeat(values, NH // KV, axis=1)
    block_rows = min(512, total)
    block_count = total // block_rows
    positions = jnp.arange(total, dtype=jnp.int32)

    def attend(pieces):
        query_block, query_seg, query_idx = pieces
        scores = low_back(jnp.einsum('qhd,khd->hqk', query_block, key_rep, precision=HIGHEST) * factor)
        scores = jnp.where(allowed(query_seg, query_idx, segment, positions)[None], scores, -1e+30)
        shifted = scores - lax.optimization_barrier(jnp.max(scores, axis=-1, keepdims=True))
        exponent = jnp.exp(shifted)
        probs = low(exponent / lax.optimization_barrier(jnp.sum(exponent, axis=-1, keepdims=True)))
        return jnp.einsum('hqk,khd->qhd', probs, value_rep, precision=HIGHEST)
    mixed = lax.map(jax.checkpoint(attend), (query_rot.reshape(block_count, block_rows, NH, HD), segment.reshape(block_count, block_rows), positions.reshape(block_count, block_rows)))
    attn_low = low(low_back(mixed.reshape(total, NH * HD)))
    branch = low_back(jnp.dot(attn_low, w_out, precision=HIGHEST))
    middle = row_input + branch
    hidden_two = low(rms_norm(middle, gain_ffn))
    gate = low_back(jnp.dot(hidden_two, w_gate, precision=HIGHEST))
    up_proj = low_back(jnp.dot(hidden_two, w_up, precision=HIGHEST))
    active = low(jax.nn.silu(gate) * up_proj)
    return middle + low_back(jnp.dot(active, w_down, precision=HIGHEST))

def reference(layer_input, grad_out, lengths, w_query, w_key, w_value, w_out, w_gate, w_up, w_down, gain_attn, gain_ffn, gain_query, gain_key):
    params = (w_query.astype(jnp.float32), w_key.astype(jnp.float32), w_value.astype(jnp.float32), w_out.astype(jnp.float32), w_gate.astype(jnp.float32), w_up.astype(jnp.float32), w_down.astype(jnp.float32), gain_attn.astype(jnp.float32), gain_ffn.astype(jnp.float32), gain_query.astype(jnp.float32), gain_key.astype(jnp.float32))
    total = layer_input.shape[1]

    def one_step(carry, inputs):
        row_input, grad_row, lengths_row = inputs
        segment, place = layout(lengths_row, total)

        def forward(rows, *weights):
            return forward_one(rows, weights, segment, place)
        result, pull = jax.vjp(forward, row_input.astype(jnp.float32), *params)
        gradients = pull(grad_row.astype(jnp.float32))
        summed = tuple((running + fresh for running, fresh in zip(carry, gradients[1:])))
        return (summed, (result.astype(jnp.bfloat16), gradients[0]))
    starting = tuple((jnp.zeros(param.shape, jnp.float32) for param in params))
    totals, (outputs, grad_inputs) = lax.scan(one_step, starting, (layer_input, grad_out, lengths))
    return (outputs, grad_inputs, totals[0], totals[1], totals[2], totals[3], totals[4], totals[5], totals[6], totals[7], totals[8], totals[9], totals[10])
```

```python
import functools
import math

import jax
import jax.numpy as jnp
from jax import lax
from jax.experimental import pallas as pl
from jax.experimental.pallas import tpu as pltpu
from jax.sharding import PartitionSpec as P

HD = 128
NDOC = 8

EPSILON = 1e-06
THETA = 1000000.0
FACTOR = 1.0 / math.sqrt(HD)
NEVER = -1e30
MESH = pl.DeviceIdType.MESH
LINE = 4
CHUNKS = 32


def rms_norm(values, gain):
    return values * lax.rsqrt(jnp.mean(values * values, axis=-1, keepdims=True) + EPSILON) * gain


def unit_rows(values):
    return values * lax.rsqrt(jnp.mean(values * values, axis=-1, keepdims=True) + EPSILON)


def rotate(values, cosine, sine):
    midway = values.shape[-1] // 2
    turned = jnp.concatenate([-values[..., midway:], values[..., :midway]], axis=-1)
    return values * cosine + turned * sine


def layout(lengths_row, total):
    finish = jnp.cumsum(lengths_row)
    starts = finish - lengths_row
    places = jnp.arange(total, dtype=jnp.int32)
    segment = jnp.sum((places[:, None] >= finish[None, :]).astype(jnp.int32), axis=1)
    member = segment[:, None] == jnp.arange(finish.shape[0], dtype=jnp.int32)[None, :]
    opening = jnp.sum(jnp.where(member, starts[None, :], 0), axis=1)
    return (segment, opening)


def angles(place):
    frequency = jnp.exp(-math.log(THETA) * jnp.arange(0, HD, 2).astype(jnp.float32) / HD)
    turning = place.astype(jnp.float32)[:, None] * frequency[None, :]
    turning = jnp.concatenate([turning, turning], axis=-1)
    return (jnp.cos(turning), jnp.sin(turning))


def tree_kernel(chunks, part, total, got_a, sum_a, got_b, a_send, a_recv, b_send, b_recv, c_send, c_recv):
    me = lax.axis_index("narrow")
    outer = (me == 0) | (me == LINE - 1)
    mate = jnp.where(me < 2, 1 - me, 5 - me)
    cross = LINE - 1 - me
    rows = part.shape[0] // chunks
    barrier = pltpu.get_barrier_semaphore()
    pl.semaphore_signal(barrier, 1, device_id={"narrow": mate}, device_id_type=MESH)

    def span(c):
        return pl.ds(pl.multiple_of(c * rows, rows), rows)

    def copy_a(c):
        return pltpu.make_async_remote_copy(
            part.at[span(c)], got_a.at[span(c)], a_send.at[c], a_recv.at[c],
            device_id={"narrow": mate}, device_id_type=MESH,
        )

    def copy_b(c):
        return pltpu.make_async_remote_copy(
            sum_a.at[span(c)], got_b.at[span(c)], b_send.at[c], b_recv.at[c],
            device_id={"narrow": cross}, device_id_type=MESH,
        )

    def copy_c(c):
        return pltpu.make_async_remote_copy(
            total.at[span(c)], total.at[span(c)], c_send.at[c], c_recv.at[c],
            device_id={"narrow": mate}, device_id_type=MESH,
        )

    @pl.when(outer)
    def _():
        pl.semaphore_wait(barrier, 1)

        @pl.loop(0, chunks)
        def _(c):
            copy_a(c).start()

        @pl.loop(0, chunks)
        def _(c):
            copy_a(c).wait_send()
            copy_c(c).wait_recv()

    @pl.when(jnp.logical_not(outer))
    def _():
        pl.semaphore_signal(barrier, 1, device_id={"narrow": cross}, device_id_type=MESH)
        pl.semaphore_wait(barrier, 2)

        def add(c):
            copy_a(c).wait_recv()
            sum_a[span(c)] = (
                part[span(c)].astype(jnp.float32) + got_a[span(c)].astype(jnp.float32)
            ).astype(jnp.bfloat16)

        def finish(c):
            copy_b(c).wait_recv()
            total[span(c)] = (
                sum_a[span(c)].astype(jnp.float32) + got_b[span(c)].astype(jnp.float32)
            ).astype(jnp.bfloat16)

        add(0)
        copy_b(0).start()

        @pl.loop(1, chunks)
        def _(c):
            add(c)
            copy_b(c).start()
            finish(c - 1)
            copy_c(c - 1).start()

        finish(chunks - 1)
        copy_c(chunks - 1).start()

        @pl.loop(0, chunks)
        def _(c):
            copy_b(c).wait_send()
            copy_c(c).wait_send()


def narrow_sum(part):
    if lax.axis_size("narrow") != LINE:
        return lax.psum(part, "narrow")
    rows, width = part.shape
    buffer = pltpu.VMEM((rows, width), jnp.bfloat16)
    semaphores = pltpu.SemaphoreType.DMA((CHUNKS,))
    return pl.pallas_call(
        functools.partial(tree_kernel, CHUNKS),
        out_shape=jax.ShapeDtypeStruct((rows, width), jnp.bfloat16),
        in_specs=[pl.BlockSpec(memory_space=pltpu.VMEM)],
        out_specs=pl.BlockSpec(memory_space=pltpu.VMEM),
        scratch_shapes=[buffer] * 3 + [semaphores] * 6,
        compiler_params=pltpu.CompilerParams(
            collective_id=0, has_side_effects=True, vmem_limit_bytes=40 << 20
        ),
        cost_estimate=pl.CostEstimate(flops=0, bytes_accessed=300_000_000, transcendentals=0),
        name="narrow_sum",
    )(part)


def contract(a, b, dims):
    return lax.dot_general(a, b, (dims, ((), ())), preferred_element_type=jnp.float32)


def attend_kernel(scalars, q_ref, k_ref, v_ref, qseg_ref, kseg_ref, o_ref, lse_ref, high, below, acc):
    own = scalars[0]
    first = scalars[1 + pl.program_id(0)]
    rows = q_ref.shape[1]
    pair = jnp.concatenate([q_ref[0, :, :HD], q_ref[0, :, HD:]], axis=0)
    qseg = jnp.concatenate([qseg_ref[0], qseg_ref[0]], axis=0)

    def raw(j):
        scores = contract(pair, k_ref[j, 0], ((1,), (1,)))
        return jnp.where(qseg == kseg_ref[0, j], scores, NEVER)

    scores = raw(own)
    upto = lax.broadcasted_iota(jnp.int32, (rows, rows), 1) <= lax.broadcasted_iota(
        jnp.int32, (rows, rows), 0
    )
    upto = jnp.concatenate([upto.astype(jnp.int32)] * 2, axis=0) != 0
    scores = jnp.where(upto, scores, NEVER)
    highest = jnp.max(scores, axis=1, keepdims=True)
    weight = jnp.exp((scores - highest) * FACTOR)
    high[...] = highest
    below[...] = jnp.sum(weight, axis=1, keepdims=True)
    acc[...] = contract(weight.astype(jnp.bfloat16), v_ref[own, 0], ((1,), (0,)))

    @pl.loop(first, own)
    def _(j):
        scores = raw(j)
        before = high[...]
        highest = jnp.maximum(before, jnp.max(scores, axis=1, keepdims=True))
        keep = jnp.exp((before - highest) * FACTOR)
        weight = jnp.exp((scores - highest) * FACTOR)
        high[...] = highest
        below[...] = below[...] * keep + jnp.sum(weight, axis=1, keepdims=True)
        acc[...] = acc[...] * keep + contract(weight.astype(jnp.bfloat16), v_ref[j, 0], ((1,), (0,)))

    mixed = (acc[...] / below[...]).astype(jnp.bfloat16)
    o_ref[0, :, :HD] = mixed[:rows]
    o_ref[0, :, HD:] = mixed[rows:]
    lse_ref[0, 0] = high[...] * FACTOR + jnp.log(below[...])


def attend(scalars, queries, keyvals, coded_own, coded):
    batch, rows, width = queries.shape
    blocks = keyvals.shape[0]
    groups = width // (2 * HD)
    return pl.pallas_call(
        attend_kernel,
        grid_spec=pltpu.PrefetchScalarGridSpec(
            num_scalar_prefetch=1,
            grid=(batch, groups),
            in_specs=[
                pl.BlockSpec((1, rows, 2 * HD), lambda m, g, s: (m, 0, g)),
                pl.BlockSpec((blocks, 1, rows, HD), lambda m, g, s: (0, m, 0, g)),
                pl.BlockSpec((blocks, 1, rows, HD), lambda m, g, s: (0, m, 0, groups + g)),
                pl.BlockSpec((1, rows, 1), lambda m, g, s: (m, 0, 0)),
                pl.BlockSpec((1, blocks, 1, rows), lambda m, g, s: (m, 0, 0, 0)),
            ],
            out_specs=[
                pl.BlockSpec((1, rows, 2 * HD), lambda m, g, s: (m, 0, g)),
                pl.BlockSpec((1, 1, 2 * rows, 1), lambda m, g, s: (m, g, 0, 0)),
            ],
            scratch_shapes=[
                pltpu.VMEM((2 * rows, 1), jnp.float32),
                pltpu.VMEM((2 * rows, 1), jnp.float32),
                pltpu.VMEM((2 * rows, HD), jnp.float32),
            ],
        ),
        out_shape=[
            jax.ShapeDtypeStruct((batch, rows, width), jnp.bfloat16),
            jax.ShapeDtypeStruct((batch, groups, 2 * rows, 1), jnp.float32),
        ],
        compiler_params=pltpu.CompilerParams(vmem_limit_bytes=48 << 20),
        cost_estimate=pl.CostEstimate(flops=4_000_000_000, bytes_accessed=12_000_000, transcendentals=4_000_000),
        name="attend",
    )(scalars, queries, keyvals, keyvals, coded_own, coded)


def attend_back_kernel(
    scalars, q_ref, kv_ref, do_ref, lse_ref, delta_ref, qseg_ref, kseg_ref, dq_ref, dkv_ref, acc
):
    own = scalars[0]
    first = scalars[1 + pl.program_id(0)]
    rows = q_ref.shape[1]
    groups = q_ref.shape[2] // (2 * HD)
    upto = lax.broadcasted_iota(jnp.int32, (rows, rows), 0) <= lax.broadcasted_iota(
        jnp.int32, (rows, rows), 1
    )
    upto = jnp.concatenate([upto.astype(jnp.int32)] * 2, axis=1) != 0
    qseg = qseg_ref[0]
    dkv_ref[...] = jnp.zeros_like(dkv_ref)
    for g in range(groups):
        left = 2 * g * HD
        pair = jnp.concatenate(
            [q_ref[0, :, left : left + HD], q_ref[0, :, left + HD : left + 2 * HD]], axis=0
        )
        dpair = jnp.concatenate(
            [do_ref[0, :, left : left + HD], do_ref[0, :, left + HD : left + 2 * HD]], axis=0
        )
        lse = lse_ref[0, g]
        delta = delta_ref[0, g]
        kcol = slice(g * HD, (g + 1) * HD)
        vcol = slice((groups + g) * HD, (groups + g + 1) * HD)

        def one(j, diagonal):
            keys = kv_ref[j, 0, :, kcol]
            scores = contract(keys, pair, ((1,), (1,))) * FACTOR
            valid = kseg_ref[0, j] == qseg
            if diagonal:
                valid = valid & upto
            probs = jnp.where(valid, jnp.exp(scores - lse), 0.0)
            dprobs = contract(kv_ref[j, 0, :, vcol], dpair, ((1,), (1,)))
            dscores = (probs * (dprobs - delta)).astype(jnp.bfloat16)
            dkv_ref[j, 0, :, kcol] = (contract(dscores, pair, ((1,), (0,))) * FACTOR).astype(jnp.bfloat16)
            dkv_ref[j, 0, :, vcol] = contract(probs.astype(jnp.bfloat16), dpair, ((1,), (0,))).astype(
                jnp.bfloat16
            )
            return contract(dscores, keys, ((0,), (0,)))

        acc[...] = one(own, True)

        @pl.loop(first, own)
        def _(j):
            acc[...] += one(j, False)

        dq_ref[0, :, left : left + HD] = acc[:rows] * FACTOR
        dq_ref[0, :, left + HD : left + 2 * HD] = acc[rows:] * FACTOR


def attend_back(scalars, queries, keyvals, grad_mixed, lse, delta, coded_own, coded):
    batch, rows, width = queries.shape
    blocks = keyvals.shape[0]
    groups = width // (2 * HD)
    row_spec = pl.BlockSpec((1, rows, width), lambda m, s: (m, 0, 0))
    all_spec = pl.BlockSpec((blocks, 1, rows, width), lambda m, s: (0, m, 0, 0))
    stat_spec = pl.BlockSpec((1, groups, 1, 2 * rows), lambda m, s: (m, 0, 0, 0))
    return pl.pallas_call(
        attend_back_kernel,
        grid_spec=pltpu.PrefetchScalarGridSpec(
            num_scalar_prefetch=1,
            grid=(batch,),
            in_specs=[
                row_spec,
                all_spec,
                row_spec,
                stat_spec,
                stat_spec,
                pl.BlockSpec((1, 1, 2 * rows), lambda m, s: (m, 0, 0)),
                pl.BlockSpec((1, blocks, rows, 1), lambda m, s: (m, 0, 0, 0)),
            ],
            out_specs=[row_spec, all_spec],
            scratch_shapes=[pltpu.VMEM((2 * rows, HD), jnp.float32)],
        ),
        out_shape=[
            jax.ShapeDtypeStruct((batch, rows, width), jnp.float32),
            jax.ShapeDtypeStruct((blocks, batch, rows, width), jnp.bfloat16),
        ],
        compiler_params=pltpu.CompilerParams(vmem_limit_bytes=56 << 20),
        cost_estimate=pl.CostEstimate(flops=10_000_000_000, bytes_accessed=24_000_000, transcendentals=4_000_000),
        name="attend_back",
    )(scalars, queries, keyvals, grad_mixed, lse, delta, coded_own, coded)


def gather_rows(shard):
    return lax.all_gather(shard, "wide", axis=0, tiled=True)


def scatter_rows(full):
    return lax.psum_scatter(
        full.astype(jnp.bfloat16), "wide", scatter_dimension=0, tiled=True
    ).astype(jnp.float32)


def scatter_columns(full):
    return lax.psum_scatter(
        full.astype(jnp.bfloat16), "wide", scatter_dimension=1, tiled=True
    ).astype(jnp.float32)


def local(
    layer_input,
    grad_out,
    lengths,
    w_query,
    w_key,
    w_value,
    w_out,
    w_gate,
    w_up,
    w_down,
    gain_attn,
    gain_ffn,
    gain_query,
    gain_key,
):
    batch, tok_rows, model = layer_input.shape
    width = lax.axis_size("wide")
    total = tok_rows * width
    rows = batch * tok_rows
    q_width, k_width, ffn = w_query.shape[1], w_key.shape[1], w_gate.shape[1]
    groups = k_width // HD
    own = lax.axis_index("wide")
    first_row = own * tok_rows
    low = jnp.bfloat16

    w_qkv = gather_rows(jnp.concatenate([w_query, w_key, w_value], axis=1))
    w_out_all = lax.all_gather(w_out, "wide", axis=1, tiled=True)

    segment, opening = jax.vmap(lambda one: layout(one, total))(lengths)
    positions = jnp.arange(total, dtype=jnp.int32)
    coded = jnp.where(segment == NDOC - 1, NDOC + positions[None, :], segment)
    coded_own = lax.dynamic_slice_in_dim(coded, first_row, tok_rows, axis=1)
    opening_own = lax.dynamic_slice_in_dim(opening, first_row, tok_rows, axis=1)
    padded = coded_own[:, 0] >= NDOC
    first = jnp.where(padded, own, opening_own[:, 0] // tok_rows)
    scalars = jnp.concatenate([own[None].astype(jnp.int32), first.astype(jnp.int32)])
    place = (first_row + jnp.arange(tok_rows, dtype=jnp.int32))[None, :] - opening_own
    cosine, sine = angles(place.reshape(rows))

    def head_norm(values, gain):
        return rotate(rms_norm(values, gain), cosine[:, None, :], sine[:, None, :])

    input_float = layer_input.reshape(rows, model).astype(jnp.float32)
    grad_low = grad_out.reshape(rows, model)
    normed_one, pull_one = jax.vjp(lambda values: rms_norm(values, gain_attn), input_float)
    hidden_one = normed_one.astype(low)
    qkv = contract(hidden_one, w_qkv, ((1,), (0,)))
    query_raw = qkv[:, :q_width].reshape(rows, q_width // HD, HD)
    key_raw = qkv[:, q_width : q_width + k_width].reshape(rows, groups, HD)
    value_low = qkv[:, q_width + k_width :].astype(low)
    query_turned, pull_query = jax.vjp(head_norm, query_raw, gain_query)
    key_turned, pull_key = jax.vjp(head_norm, key_raw, gain_key)
    query_low = query_turned.astype(low).reshape(batch, tok_rows, q_width)
    key_low = key_turned.astype(low).reshape(rows, k_width)
    keyvals = jnp.concatenate([key_low, value_low], axis=1).reshape(batch, tok_rows, 2 * k_width)
    keyvals = lax.all_gather(keyvals, "wide", axis=0, tiled=False)

    w_gate_up = gather_rows(jnp.concatenate([w_gate, w_up], axis=1))
    w_down_all = lax.all_gather(w_down, "wide", axis=1, tiled=True)

    coded_blocks = coded.reshape(batch, width, tok_rows)
    mixed_low, lse = attend(
        scalars, query_low, keyvals, coded_own[:, :, None], coded_blocks[:, :, None, :]
    )
    mixed_flat = mixed_low.reshape(rows, q_width)
    attn_part = contract(mixed_flat, w_out_all, ((1,), (0,))).astype(low)
    middle = input_float + narrow_sum(attn_part).astype(jnp.float32)
    normed_two, pull_two = jax.vjp(lambda values: rms_norm(values, gain_ffn), middle)
    hidden_two = normed_two.astype(low)

    gate_up = contract(hidden_two, w_gate_up, ((1,), (0,)))
    gate, up_proj = gate_up[:, :ffn], gate_up[:, ffn:]
    grad_active = contract(grad_low, w_down_all, ((1,), (1,)))
    active, pull_active = jax.vjp(lambda g, u: jax.nn.silu(g) * u, gate, up_proj)
    active_low = active.astype(low)
    grad_gate, grad_upper = pull_active(grad_active)
    ffn_back = jnp.concatenate([grad_gate.astype(low), grad_upper.astype(low)], axis=1)
    partial_two = contract(ffn_back, w_gate_up, ((1,), (1,)))
    gain_two = jnp.sum(partial_two * unit_rows(middle), axis=0)
    ffn_part = contract(active_low, w_down_all, ((1,), (0,))).astype(low)
    grad_wgate_up = scatter_rows(contract(hidden_two, ffn_back, ((0,), (0,))))
    grad_wdown = scatter_columns(contract(active_low, grad_low, ((0,), (0,))))

    grad_middle = grad_low.astype(jnp.float32) + pull_two(
        narrow_sum(partial_two.astype(low)).astype(jnp.float32)
    )[0]
    middle_low = grad_middle.astype(low)
    grad_mixed = contract(middle_low, w_out_all, ((1,), (1,)))
    grad_mixed = grad_mixed.astype(low)
    grad_wout = scatter_columns(contract(mixed_flat, middle_low, ((0,), (0,))))
    heads = q_width // HD
    delta = jnp.sum(
        (grad_mixed.astype(jnp.float32) * mixed_flat.astype(jnp.float32)).reshape(
            batch, tok_rows, heads, HD
        ),
        axis=-1,
    )
    delta = delta.transpose(0, 2, 1).reshape(batch, groups, 1, 2 * tok_rows)
    coded_pair = jnp.concatenate([coded_own, coded_own], axis=1)[:, None, :]
    grad_turned, grad_keyvals = attend_back(
        scalars,
        query_low,
        keyvals,
        grad_mixed.reshape(batch, tok_rows, q_width),
        lse.reshape(batch, groups, 1, 2 * tok_rows),
        delta,
        coded_pair,
        coded_blocks[:, :, :, None],
    )
    grad_keyvals = lax.psum_scatter(grad_keyvals, "wide", scatter_dimension=0, tiled=False)
    grad_keyvals = grad_keyvals.reshape(rows, 2 * k_width)
    grad_keys = grad_keyvals[:, :k_width].astype(jnp.float32)
    value_back = grad_keyvals[:, k_width:]

    output = (middle + narrow_sum(ffn_part).astype(jnp.float32)).astype(low)

    grad_qraw, gain_q = pull_query(grad_turned.reshape(rows, heads, HD))
    grad_kraw, gain_k = pull_key(grad_keys.reshape(rows, groups, HD))
    back = jnp.concatenate(
        [
            grad_qraw.reshape(rows, q_width).astype(low),
            grad_kraw.reshape(rows, k_width).astype(low),
            value_back,
        ],
        axis=1,
    )
    partial_one = contract(back, w_qkv, ((1,), (1,)))
    gain_one = jnp.sum(partial_one * unit_rows(input_float), axis=0)
    grad_wqkv = scatter_rows(contract(hidden_one, back, ((0,), (0,))))
    gain_total = lax.psum((gain_one, gain_two, gain_q, gain_k), ("wide", "narrow"))
    grad_input = (
        grad_middle + pull_one(narrow_sum(partial_one.astype(low)).astype(jnp.float32))[0]
    )
    return (
        output.reshape(batch, tok_rows, model),
        grad_input.reshape(batch, tok_rows, model),
        grad_wqkv[:, :q_width],
        grad_wqkv[:, q_width : q_width + k_width],
        grad_wqkv[:, q_width + k_width :],
        grad_wout,
        grad_wgate_up[:, :ffn],
        grad_wgate_up[:, ffn:],
        grad_wdown,
    ) + gain_total


def solution(mesh):
    in_specs = (
        P(None, "wide", None),
        P(None, "wide", None),
        P(),
        P("wide", "narrow"),
        P("wide", "narrow"),
        P("wide", "narrow"),
        P("narrow", "wide"),
        P("wide", "narrow"),
        P("wide", "narrow"),
        P("narrow", "wide"),
        P(),
        P(),
        P(),
        P(),
    )
    out_specs = (
        P(None, "wide", None),
        P(None, "wide", None),
        P("wide", "narrow"),
        P("wide", "narrow"),
        P("wide", "narrow"),
        P("narrow", "wide"),
        P("wide", "narrow"),
        P("wide", "narrow"),
        P("narrow", "wide"),
        P(),
        P(),
        P(),
        P(),
    )
    return jax.shard_map(local, mesh=mesh, in_specs=in_specs, out_specs=out_specs, check_vma=False)
```
